32 devices in a mesh: replica: 2 (over x), seq: 16 (over z, y, core).
Axes of the slice: x: 2, y: 2, z: 4, core: 2. Of those that a mesh axis runs over, the one named last changes fastest.
Arguments:
- hidden_in: bfloat16 [32, 8192], P('replica'), parts along dimension 0, may hold values from -6 to 6
- w_query: bfloat16 [8192, 8192], P(None, 'seq'), may hold values from -1 to 1
- w_keyval: bfloat16 [8192, 2048], P(None, 'seq'), may hold values from -0.1875 to 0.1875
- key_cache: bfloat16 [32, 2048, 1024], P('replica', 'seq'), parts along dimension 0, may hold values from -15 to 15
- value_cache: bfloat16 [32, 2048, 1024], P('replica', 'seq'), parts along dimension 0, may hold values from -6 to 6
- lengths: int32 [32], P('replica'), parts along dimension 0, may hold values from 128 to 2047, as said below
- w_out: bfloat16 [8192, 8192], P('seq'), may hold values from -0.09375 to 0.09375
Outputs:
- attn_out: bfloat16 [32, 8192], P('replica', 'seq'), parts along dimension 0
The draws below stay inside these ranges and needn't reach their ends.
There are 2 independent parts, one for each index of `replica`. The reference program is written for one: setup_inputs(seed, part) draws one part's arguments, and reference() takes and returns one part's arrays. A program takes and returns all parts, laid end to end along the dimension named above; an argument that names none is the same for every part. Nothing has to cross between parts.
Inputs may be any that keep to these rules, and one draw needn't show every extreme that they name: The new token of sequence b is written at position lengths[b]; it attends to positions 0 to lengths[b].
All inputs are finite; a program needn't handle non-finite values.
Results may differ from the reference program's by a relative error of at most 0.013.
Values may be sent and summed in bfloat16 or wider, within the bound.
A program may use at most 64 MiB of HBM per device.

```python
import math
import jax
import jax.numpy as jnp
from jax import lax

D = 8192
HEADS = 64
KV_HEADS = 8
HEAD_DIM = 128
BATCH = 16
CTX_DEV = 128
CTX = 2048


def plan_draw(key):
    lengths = jax.random.randint(jax.random.fold_in(key, 101), (BATCH,), CTX_DEV, CTX, dtype=jnp.int32)
    return lengths


def draw_lengths(key, part):
    return plan_draw(key)


def draw_hidden_in(key, part):
    base = jnp.clip(jax.random.normal(jax.random.fold_in(key, 1), (BATCH, D), jnp.float32), -6.0, 6.0)
    return base.astype(jnp.bfloat16)


def draw_w_query(key, part):
    width = HEADS * HEAD_DIM
    scale = 1.0 / math.sqrt(D)
    base = jnp.clip(jax.random.normal(key, (D, width), jnp.float32), -6.0, 6.0) * scale
    return base.astype(jnp.bfloat16)


def draw_key_cache(key, part):
    width = KV_HEADS * HEAD_DIM
    base = jnp.clip(jax.random.normal(jax.random.fold_in(key, 2), (BATCH, CTX, width), jnp.float32), -15.0, 15.0)
    return base.astype(jnp.bfloat16)


def raised(result, rng, source, target, shards_of, factor):
    def block_of(dim):
        return (jnp.arange(result.shape[dim]) // (result.shape[dim] // shards_of)).reshape((-1,) + (1,) * (result.ndim - 1 - dim))

    first = jax.random.permutation(rng, shards_of)[block_of(target)]
    other_side = (block_of(target) + shards_of // 2) % shards_of
    return jnp.where((block_of(source) == first) | (block_of(source) == other_side), factor * result, result)


def shard_levels(rng, shape, shards, low, top_value):
    gain = 1.0
    for dim, blocks in shards:
        heights = jax.random.uniform(jax.random.fold_in(jax.random.fold_in(rng, 6), dim), (blocks,), jnp.float32, low / len(shards), top_value / len(shards))
        gain = gain * jnp.repeat(jnp.exp(heights), shape[dim] // blocks).reshape((-1,) + (1,) * (len(shape) - 1 - dim))
    return gain


def normal_values(rng, shape, scale, reach, shards=(), kind=jnp.bfloat16):
    values = scale * jax.random.normal(rng, shape, jnp.float32)
    if shards:
        values = values * shard_levels(rng, shape, shards, -0.22, 0.18)
    return jnp.clip(values, -reach, reach).astype(kind)


def gaussian_with(key, shape, scale, limit, shards, heavy, kind=jnp.bfloat16):
    entries = scale * jax.random.normal(key, shape, jnp.float32)
    if shards:
        entries = entries * shard_levels(key, shape, shards, -0.22, 0.18)
    return jnp.clip(raised(entries, jax.random.fold_in(key, 3), *heavy), -limit, limit).astype(kind)


def setup_inputs(seed: int = 0, part: int = 0) -> dict:
    keys = jax.random.split(jax.random.key(seed), 8)
    part_splits = jax.random.split(jax.random.fold_in(keys[7], part), 8)
    return {
        "hidden_in": draw_hidden_in(jax.random.fold_in(jax.random.fold_in(keys[7], part), 71), part),
        "w_query": draw_w_query(jax.random.fold_in(keys[7], 71), part),
        "w_keyval": normal_values(keys[2], (D, 2 * KV_HEADS * HEAD_DIM), (D // 9) ** -0.5, 0.1875, ((1, 16),)),
        "key_cache": draw_key_cache(jax.random.fold_in(jax.random.fold_in(keys[7], part), 71), part),
        "value_cache": normal_values(part_splits[4], (BATCH, CTX, KV_HEADS * HEAD_DIM), 1.0, 6.0, ((1, 16),)),
        "lengths": draw_lengths(jax.random.fold_in(jax.random.fold_in(keys[7], part), 71), part),
        "w_out": gaussian_with(keys[6], (HEADS * HEAD_DIM, D), (HEADS * HEAD_DIM) ** -0.5, 0.09375, ((0, 16),), (0, 1, 16, 2.0)),
    }


def reference(hidden_in, w_query, w_keyval, key_cache, value_cache, lengths, w_out):
    query = jnp.dot(hidden_in, w_query, preferred_element_type=jnp.float32).astype(jnp.bfloat16)
    new_kv = jnp.dot(hidden_in, w_keyval, preferred_element_type=jnp.float32).astype(jnp.bfloat16)
    half_width = KV_HEADS * HEAD_DIM
    group_size = HEADS // KV_HEADS

    def attend(sequence):
        query_row, new_key, new_value, cached_keys, cached_values, position = sequence
        anchor = (position.astype(jnp.int32), jnp.int32(0))
        key_rows = lax.dynamic_update_slice(cached_keys, new_key[None, :], anchor)
        value_rows = lax.dynamic_update_slice(cached_values, new_value[None, :], anchor)
        query_f32 = query_row.astype(jnp.float32).reshape(KV_HEADS, group_size, HEAD_DIM)
        key_f32 = key_rows.astype(jnp.float32).reshape(CTX, KV_HEADS, HEAD_DIM)
        scores = jnp.einsum('kgd,tkd->kgt', query_f32, key_f32) / math.sqrt(HEAD_DIM)
        positions = jnp.arange(CTX, dtype=jnp.int32)
        scores = jnp.where(positions <= position, scores, -1e+30)
        largest = lax.optimization_barrier(jnp.max(scores, axis=-1))
        weights = jnp.exp(scores - largest[..., None])
        total = lax.optimization_barrier(jnp.sum(weights, axis=-1))
        rounded = lax.optimization_barrier(weights.astype(jnp.bfloat16)).astype(jnp.float32)
        value_f32 = value_rows.astype(jnp.float32).reshape(CTX, KV_HEADS, HEAD_DIM)
        summed = jnp.einsum('kgt,tkd->kgd', rounded, value_f32)
        return (summed / total[..., None]).reshape(HEADS * HEAD_DIM)
    attended = lax.map(attend, (query, new_kv[:, :half_width], new_kv[:, half_width:], key_cache, value_cache, lengths))
    attended = attended.astype(jnp.bfloat16)
    return jnp.dot(attended, w_out, preferred_element_type=jnp.float32).astype(jnp.bfloat16)
```

```python
import functools
import math

import jax
import jax.numpy as jnp
from jax import lax
from jax.experimental import pallas as pl
from jax.experimental.pallas import tpu as pltpu
from jax.sharding import PartitionSpec as P

KV_HEADS = 8
HEAD_DIM = 128
LANES = 128
MESH = pl.DeviceIdType.MESH
F32 = jnp.float32
BF16 = jnp.bfloat16


def kernel(
    shards, chunks,
    x_hbm, wq_hbm, wkv_hbm, kc_hbm, vc_hbm, len_ref, wo_hbm,
    out_ref,
    x_v, wq_v, wkv_v, kc_v, vc_v, wo_v,
    q_all, kv_s, kv_r, qf, of, lf, part_s, part_r, att_v, term_s, term_r,
    x_sem, wq_sem, wkv_sem, kc_sem, vc_sem, wo_sem,
    q_send, q_recv, kv_send, kv_recv, p_send, p_recv, t_send, t_recv,
):
    me = lax.axis_index("seq")
    batch, ctx_dev = kc_v.shape[0], kc_v.shape[1]
    depth = x_v.shape[1]
    width = q_all.shape[2]
    heads_dev = width // HEAD_DIM
    owners = shards // KV_HEADS
    group = owners * heads_dev
    kv_cols = kv_s.shape[1]
    pieces = HEAD_DIM // kv_cols
    step = depth // chunks
    region = LANES // heads_dev

    x_copy = pltpu.make_async_copy(x_hbm, x_v, x_sem)
    x_copy.start()
    wq_copies, wkv_copies = [], []
    for c in range(chunks):
        rows = pl.ds(c * step, step)
        wq_copies.append(pltpu.make_async_copy(wq_hbm.at[rows], wq_v.at[rows], wq_sem.at[c]))
        wkv_copies.append(pltpu.make_async_copy(wkv_hbm.at[rows], wkv_v.at[rows], wkv_sem.at[c]))
        wq_copies[c].start()
        wkv_copies[c].start()
    kc_copy = pltpu.make_async_copy(kc_hbm, kc_v, kc_sem)
    vc_copy = pltpu.make_async_copy(vc_hbm, vc_v, vc_sem)
    wo_copy = pltpu.make_async_copy(wo_hbm, wo_v, wo_sem)

    barrier = pltpu.get_barrier_semaphore()

    def greet(i, carry):
        pl.semaphore_signal(
            barrier, inc=1, device_id={"seq": lax.rem(me + i, shards)}, device_id_type=MESH
        )
        return carry

    lax.fori_loop(1, shards, greet, 0)

    acc_q = jnp.zeros((batch, width), F32)
    acc_kv = jnp.zeros((batch, kv_cols), F32)
    x_copy.wait()
    for c in range(chunks):
        wq_copies[c].wait()
        wkv_copies[c].wait()
        part = x_v[:, c * step:(c + 1) * step]
        acc_q += jnp.dot(part, wq_v[c * step:(c + 1) * step, :], preferred_element_type=F32)
        acc_kv += jnp.dot(part, wkv_v[c * step:(c + 1) * step, :], preferred_element_type=F32)
        if c == chunks // 2:
            kc_copy.start()
            vc_copy.start()
            wo_copy.start()
    q_all[me] = acc_q.astype(BF16)
    kv_s[...] = acc_kv.astype(BF16)

    pl.semaphore_wait(barrier, shards - 1)

    def q_copy(slot, peer):
        return pltpu.make_async_remote_copy(
            src_ref=q_all.at[slot], dst_ref=q_all.at[slot],
            send_sem=q_send.at[peer], recv_sem=q_recv.at[slot],
            device_id={"seq": peer}, device_id_type=MESH,
        )

    def send_q(i, carry):
        q_copy(me, lax.rem(me + i, shards)).start()
        return carry

    lax.fori_loop(1, shards, send_q, 0)

    half = shards // 2
    role = me // half
    within = me - role * half
    my_head = within // pieces
    my_slot = role * pieces + (within - my_head * pieces)

    def kv_copy(slot, peer, g):
        return pltpu.make_async_remote_copy(
            src_ref=kv_s, dst_ref=kv_r.at[slot],
            send_sem=kv_send.at[g], recv_sem=kv_recv.at[slot],
            device_id={"seq": peer}, device_id_type=MESH,
        )

    def kv_local():
        return pltpu.make_async_copy(kv_s, kv_r.at[my_slot], kv_recv.at[my_slot])

    for g in range(owners):
        peer = my_head * owners + g

        @pl.when(peer != me)
        def _():
            kv_copy(my_slot, peer, g).start()

        @pl.when(peer == me)
        def _():
            kv_local().start()

    kc_copy.wait()
    vc_copy.wait()

    first = me * ctx_dev
    scale = 1.0 / math.sqrt(HEAD_DIM)
    my_group = me // owners
    slots = lax.broadcasted_iota(jnp.int32, (group, ctx_dev), 1) + first
    lane = lax.broadcasted_iota(jnp.int32, (batch, LANES), 1)

    def part_copy(src_slot, dst_slot, peer):
        return pltpu.make_async_remote_copy(
            src_ref=part_s.at[src_slot], dst_ref=part_r.at[dst_slot],
            send_sem=p_send.at[peer], recv_sem=p_recv.at[dst_slot],
            device_id={"seq": peer}, device_id_type=MESH,
        )

    def part_local():
        return pltpu.make_async_copy(part_s.at[me], part_r.at[me], p_recv.at[me])

    def attend(i, carry):
        k = lax.rem(my_group + i, KV_HEADS)
        cols = pl.ds(pl.multiple_of(k * HEAD_DIM, HEAD_DIM), HEAD_DIM)
        for g in range(owners):
            src = k * owners + g

            @pl.when(src != me)
            def _():
                q_copy(src, src).wait_recv()

        for g in range(owners):
            block = q_all[k * owners + g].astype(F32)
            for h in range(heads_dev):
                qf[:, g * heads_dev + h, :] = block[:, h * HEAD_DIM:(h + 1) * HEAD_DIM]
        for b in range(batch):
            scores = lax.dot_general(
                qf[b].astype(BF16), kc_v[b, :, cols], (((1,), (1,)), ((), ())),
                preferred_element_type=F32,
            ) * scale
            scores = jnp.where(slots < len_ref[b], scores, -1e30)
            largest = jnp.max(scores, axis=-1, keepdims=True)
            weights = jnp.exp(scores - largest)
            total = jnp.sum(weights, axis=-1, keepdims=True)
            summed = jnp.dot(weights.astype(BF16), vc_v[b, :, cols], preferred_element_type=F32)
            of[b] = summed / total
            lf[b] = jnp.broadcast_to(largest + jnp.log(total), (group, LANES))
        for g in range(owners):
            d = k * owners + g
            stats = jnp.zeros((batch, LANES), F32)
            for h in range(heads_dev):
                part_s[d, :, h * HEAD_DIM:(h + 1) * HEAD_DIM] = of[:, g * heads_dev + h, :].astype(BF16)
                lse = lf[:, g * heads_dev + h, :]
                high = lse.astype(BF16).astype(F32)
                mid = (lse - high).astype(BF16).astype(F32)
                low = lse - high - mid
                base = h * region
                stats = jnp.where(lane == base, high, stats)
                stats = jnp.where(lane == base + 1, mid, stats)
                stats = jnp.where(lane == base + 2, low, stats)
            part_s[d, :, width:] = stats.astype(BF16)

            @pl.when(d != me)
            def _():
                part_copy(d, me, d).start()

            @pl.when(d == me)
            def _():
                part_local().start()

        return carry

    lax.fori_loop(0, KV_HEADS, attend, 0)

    owner_head = me // owners
    for r in range(2 * pieces):
        src = (r // pieces) * half + owner_head * pieces + r % pieces

        @pl.when(src != me)
        def _():
            kv_copy(r, src, 0).wait_recv()

        @pl.when(src == me)
        def _():
            kv_local().wait()

    def wait_part(i, carry):
        part_copy(lax.rem(me + i, shards), lax.rem(me + i, shards), lax.rem(me + i, shards)).wait_recv()
        return carry

    lax.fori_loop(1, shards, wait_part, 0)
    part_local().wait()

    def lse_of(s, h):
        stats = part_r[s, :, width:].astype(F32)
        mine = (lane >= h * region) & (lane < (h + 1) * region)
        return jnp.sum(jnp.where(mine, stats, 0.0), axis=-1, keepdims=True)

    new_value = jnp.concatenate([kv_r[pieces + p].astype(F32) for p in range(pieces)], axis=-1)
    new_key = jnp.concatenate([kv_r[p].astype(F32) for p in range(pieces)], axis=-1)
    own_q = q_all[me].astype(F32)
    fresh = [
        jnp.sum(own_q[:, h * HEAD_DIM:(h + 1) * HEAD_DIM] * new_key, axis=-1, keepdims=True) * scale
        for h in range(heads_dev)
    ]

    def top_of(s, tops):
        return tuple(jnp.maximum(t, lse_of(s, h)) for h, t in enumerate(tops))

    tops = lax.fori_loop(0, shards, top_of, tuple(fresh))
    shares = [jnp.exp(f - t) for f, t in zip(fresh, tops)]

    def merge(s, state):
        sums, totals = state
        new_sums, new_totals = [], []
        for h in range(heads_dev):
            share = jnp.exp(lse_of(s, h) - tops[h])
            values = part_r[s, :, h * HEAD_DIM:(h + 1) * HEAD_DIM].astype(F32)
            new_sums.append(sums[h] + share * values)
            new_totals.append(totals[h] + share)
        return tuple(new_sums), tuple(new_totals)

    sums, totals = lax.fori_loop(
        0, shards, merge, (tuple(s * new_value for s in shares), tuple(shares))
    )
    for h in range(heads_dev):
        att_v[:, h * HEAD_DIM:(h + 1) * HEAD_DIM] = (sums[h] / totals[h]).astype(BF16)

    wo_copy.wait()
    out_cols = term_s.shape[2]

    def term_copy(src_slot, dst_slot, peer):
        return pltpu.make_async_remote_copy(
            src_ref=term_s.at[src_slot], dst_ref=term_r.at[dst_slot],
            send_sem=t_send.at[peer], recv_sem=t_recv.at[dst_slot],
            device_id={"seq": peer}, device_id_type=MESH,
        )

    def term_of(d):
        cols = pl.ds(pl.multiple_of(d * out_cols, out_cols), out_cols)
        return jnp.dot(att_v[...], wo_v[:, cols], preferred_element_type=F32)

    def project(i, carry):
        d = lax.rem(me + i, shards)
        term_s[d] = term_of(d).astype(BF16)
        term_copy(d, me, d).start()
        return carry

    lax.fori_loop(1, shards, project, 0)
    own = term_of(me)

    def collect(i, total):
        s = lax.rem(me + i, shards)
        term_copy(s, s, s).wait_recv()
        return total + term_r[s].astype(F32)

    out_ref[...] = lax.fori_loop(1, shards, collect, own).astype(BF16)

    def drain(i, carry):
        peer = lax.rem(me + i, shards)
        q_copy(me, peer).wait_send()
        part_copy(peer, peer, peer).wait_send()
        term_copy(peer, peer, peer).wait_send()
        return carry

    lax.fori_loop(1, shards, drain, 0)
    for g in range(owners):
        peer = my_head * owners + g

        @pl.when(peer != me)
        def _():
            kv_copy(my_slot, peer, g).wait_send()


def body(hidden_in, w_query, w_keyval, key_cache, value_cache, lengths, w_out):
    shards = lax.axis_size("seq")
    batch, depth = hidden_in.shape
    width = w_query.shape[1]
    kv_cols = w_keyval.shape[1]
    heads_dev = width // HEAD_DIM
    owners = shards // KV_HEADS
    group = owners * heads_dev
    pieces = HEAD_DIM // kv_cols
    out_cols = w_out.shape[1] // shards
    chunks = 8
    dma = pltpu.SemaphoreType.DMA
    hbm = pl.BlockSpec(memory_space=pl.ANY)
    return pl.pallas_call(
        functools.partial(kernel, shards, chunks),
        out_shape=jax.ShapeDtypeStruct((batch, out_cols), BF16),
        in_specs=[hbm, hbm, hbm, hbm, hbm, pl.BlockSpec(memory_space=pltpu.SMEM), hbm],
        out_specs=pl.BlockSpec(memory_space=pltpu.VMEM),
        scratch_shapes=[
            pltpu.VMEM(hidden_in.shape, BF16),
            pltpu.VMEM(w_query.shape, BF16),
            pltpu.VMEM(w_keyval.shape, BF16),
            pltpu.VMEM(key_cache.shape, BF16),
            pltpu.VMEM(value_cache.shape, BF16),
            pltpu.VMEM(w_out.shape, BF16),
            pltpu.VMEM((shards, batch, width), BF16),
            pltpu.VMEM((batch, kv_cols), BF16),
            pltpu.VMEM((2 * pieces, batch, kv_cols), BF16),
            pltpu.VMEM((batch, group, HEAD_DIM), F32),
            pltpu.VMEM((batch, group, HEAD_DIM), F32),
            pltpu.VMEM((batch, group, LANES), F32),
            pltpu.VMEM((shards, batch, width + LANES), BF16),
            pltpu.VMEM((shards, batch, width + LANES), BF16),
            pltpu.VMEM((batch, width), BF16),
            pltpu.VMEM((shards, batch, out_cols), BF16),
            pltpu.VMEM((shards, batch, out_cols), BF16),
            dma, dma((chunks,)), dma((chunks,)), dma, dma, dma,
            dma((shards,)), dma((shards,)), dma((owners,)), dma((2 * pieces,)),
            dma((shards,)), dma((shards,)), dma((shards,)), dma((shards,)),
        ],
        compiler_params=pltpu.CompilerParams(
            collective_id=0, has_side_effects=True, vmem_limit_bytes=60 * 1024 * 1024
        ),
    )(hidden_in, w_query, w_keyval, key_cache, value_cache, lengths, w_out)


def solution(mesh):
    placed = (
        P("replica", None),
        P(None, "seq"),
        P(None, "seq"),
        P("replica", "seq", None),
        P("replica", "seq", None),
        P("replica"),
        P("seq", None),
    )
    return jax.shard_map(
        body, mesh=mesh, in_specs=placed, out_specs=P("replica", "seq"), check_vma=False
    )
```

```python
import functools
import math

import jax
import jax.numpy as jnp
from jax import lax
from jax.experimental import pallas as pl
from jax.experimental.pallas import tpu as pltpu
from jax.sharding import PartitionSpec as P

KV_HEADS = 8
HEAD_DIM = 128
LANES = 128
PAIR = 2
MESH = pl.DeviceIdType.MESH
F32 = jnp.float32
BF16 = jnp.bfloat16


def kernel(
    shards, chunks,
    x_hbm, wq_hbm, wkv_hbm, kc_hbm, vc_hbm, len_ref, wo_hbm,
    out_ref,
    x_v, wq_v, wkv_v, kc_v, vc_v, wo_v,
    q_all, kv_s, kv_r, qf, of, lf, part_s, part_r, att_v, term_s, term_r,
    x_sem, wq_sem, wkv_sem, kc_sem, vc_sem, wo_sem,
    q_send, q_recv, kv_send, kv_recv, p_send, p_recv, t_send, t_recv,
):
    me = lax.axis_index("seq")
    batch, ctx_dev = kc_v.shape[0], kc_v.shape[1]
    depth = x_v.shape[1]
    width = q_all.shape[2]
    heads_dev = width // HEAD_DIM
    owners = shards // KV_HEADS
    group = owners * heads_dev
    kv_cols = kv_s.shape[1]
    pieces = HEAD_DIM // kv_cols
    step = depth // chunks
    region = LANES // heads_dev

    x_copy = pltpu.make_async_copy(x_hbm, x_v, x_sem)
    x_copy.start()
    wq_copies, wkv_copies = [], []
    for c in range(chunks):
        rows = pl.ds(c * step, step)
        wq_copies.append(pltpu.make_async_copy(wq_hbm.at[rows], wq_v.at[rows], wq_sem.at[c]))
        wkv_copies.append(pltpu.make_async_copy(wkv_hbm.at[rows], wkv_v.at[rows], wkv_sem.at[c]))
        wq_copies[c].start()
        wkv_copies[c].start()
    kc_copy = pltpu.make_async_copy(kc_hbm, kc_v, kc_sem)
    vc_copy = pltpu.make_async_copy(vc_hbm, vc_v, vc_sem)
    wo_copy = pltpu.make_async_copy(wo_hbm, wo_v, wo_sem)

    barrier = pltpu.get_barrier_semaphore()

    def greet(i, carry):
        pl.semaphore_signal(
            barrier, inc=1, device_id={"seq": lax.rem(me + i, shards)}, device_id_type=MESH
        )
        return carry

    lax.fori_loop(1, shards, greet, 0)

    acc_q = jnp.zeros((batch, width), F32)
    acc_kv = jnp.zeros((batch, kv_cols), F32)
    x_copy.wait()
    for c in range(chunks):
        wq_copies[c].wait()
        wkv_copies[c].wait()
        part = x_v[:, c * step:(c + 1) * step]
        acc_q += jnp.dot(part, wq_v[c * step:(c + 1) * step, :], preferred_element_type=F32)
        acc_kv += jnp.dot(part, wkv_v[c * step:(c + 1) * step, :], preferred_element_type=F32)
        if c == chunks // 2:
            kc_copy.start()
            vc_copy.start()
            wo_copy.start()
    q_all[me] = acc_q.astype(BF16)
    kv_s[...] = acc_kv.astype(BF16)

    pl.semaphore_wait(barrier, shards - 1)

    def q_copy(slot, peer):
        return pltpu.make_async_remote_copy(
            src_ref=q_all.at[slot], dst_ref=q_all.at[slot],
            send_sem=q_send.at[peer], recv_sem=q_recv.at[slot],
            device_id={"seq": peer}, device_id_type=MESH,
        )

    def send_q(i, carry):
        q_copy(me, lax.rem(me + i, shards)).start()
        return carry

    lax.fori_loop(1, shards, send_q, 0)

    half = shards // 2
    role = me // half
    within = me - role * half
    my_head = within // pieces
    my_slot = role * pieces + (within - my_head * pieces)

    def kv_copy(slot, peer, g):
        return pltpu.make_async_remote_copy(
            src_ref=kv_s, dst_ref=kv_r.at[slot],
            send_sem=kv_send.at[g], recv_sem=kv_recv.at[slot],
            device_id={"seq": peer}, device_id_type=MESH,
        )

    def kv_local():
        return pltpu.make_async_copy(kv_s, kv_r.at[my_slot], kv_recv.at[my_slot])

    for g in range(owners):
        peer = my_head * owners + g

        @pl.when(peer != me)
        def _():
            kv_copy(my_slot, peer, g).start()

        @pl.when(peer == me)
        def _():
            kv_local().start()

    kc_copy.wait()
    vc_copy.wait()

    first = me * ctx_dev
    scale = 1.0 / math.sqrt(HEAD_DIM)
    my_group = me // owners
    slots = lax.broadcasted_iota(jnp.int32, (PAIR * group, ctx_dev), 1) + first
    used = jnp.stack([slots < len_ref[b] for b in range(batch)])
    row_head = lax.broadcasted_iota(jnp.int32, (PAIR * group, HEAD_DIM), 0) // group
    lane = lax.broadcasted_iota(jnp.int32, (batch, LANES), 1)

    def part_copy(src_slot, dst_slot, peer):
        return pltpu.make_async_remote_copy(
            src_ref=part_s.at[src_slot], dst_ref=part_r.at[dst_slot],
            send_sem=p_send.at[peer], recv_sem=p_recv.at[dst_slot],
            device_id={"seq": peer}, device_id_type=MESH,
        )

    def part_local():
        return pltpu.make_async_copy(part_s.at[me], part_r.at[me], p_recv.at[me])

    def attend(i, carry):
        pair = lax.rem(my_group // PAIR + i, KV_HEADS // PAIR)
        cols = pl.ds(pl.multiple_of(pair * PAIR * HEAD_DIM, PAIR * HEAD_DIM), PAIR * HEAD_DIM)
        devices = PAIR * owners

        def wait_q(g, c):
            src = pair * devices + g

            @pl.when(src != me)
            def _():
                q_copy(src, src).wait_recv()

            return c

        lax.fori_loop(0, devices, wait_q, 0)
        for g in range(devices):
            block = q_all[pair * devices + g].astype(F32)
            for h in range(heads_dev):
                qf[:, g * heads_dev + h, :] = block[:, h * HEAD_DIM:(h + 1) * HEAD_DIM]
        scores = []
        for b in range(batch):
            rows = qf[b]
            wide = jnp.concatenate(
                [jnp.where(row_head == n, rows, 0.0) for n in range(PAIR)], axis=1
            )
            scores.append(lax.dot_general(
                wide.astype(BF16), kc_v[b, :, cols], (((1,), (1,)), ((), ())),
                preferred_element_type=F32,
            ))
        scores = jnp.where(used, jnp.stack(scores) * scale, -1e30)
        largest = jnp.max(scores, axis=-1, keepdims=True)
        weights = jnp.exp(scores - largest)
        total = jnp.sum(weights, axis=-1, keepdims=True)
        lf[...] = jnp.broadcast_to(largest + jnp.log(total), lf.shape)
        inverse = 1.0 / total
        weights = weights.astype(BF16)
        for b in range(batch):
            summed = jnp.dot(weights[b], vc_v[b, :, cols], preferred_element_type=F32)
            mine = [
                summed[n * group:(n + 1) * group, n * HEAD_DIM:(n + 1) * HEAD_DIM]
                for n in range(PAIR)
            ]
            of[b] = jnp.concatenate(mine, axis=0) * inverse[b]
        for g in range(devices):
            d = pair * devices + g
            stats = jnp.zeros((batch, LANES), F32)
            for h in range(heads_dev):
                part_s[d, :, h * HEAD_DIM:(h + 1) * HEAD_DIM] = of[:, g * heads_dev + h, :].astype(BF16)
                lse = lf[:, g * heads_dev + h, :]
                high = lse.astype(BF16).astype(F32)
                mid = (lse - high).astype(BF16).astype(F32)
                low = lse - high - mid
                base = h * region
                stats = jnp.where(lane == base, high, stats)
                stats = jnp.where(lane == base + 1, mid, stats)
                stats = jnp.where(lane == base + 2, low, stats)
            part_s[d, :, width:] = stats.astype(BF16)

        def send_part(g, c):
            d = pair * devices + g

            @pl.when(d != me)
            def _():
                part_copy(d, me, d).start()

            @pl.when(d == me)
            def _():
                part_local().start()

            return c

        lax.fori_loop(0, devices, send_part, 0)
        return carry

    lax.fori_loop(0, KV_HEADS // PAIR, attend, 0)

    owner_head = me // owners
    for r in range(2 * pieces):
        src = (r // pieces) * half + owner_head * pieces + r % pieces

        @pl.when(src != me)
        def _():
            kv_copy(r, src, 0).wait_recv()

        @pl.when(src == me)
        def _():
            kv_local().wait()

    def wait_part(i, carry):
        part_copy(lax.rem(me + i, shards), lax.rem(me + i, shards), lax.rem(me + i, shards)).wait_recv()
        return carry

    lax.fori_loop(1, shards, wait_part, 0)
    part_local().wait()

    def lse_of(s, h):
        stats = part_r[s, :, width:].astype(F32)
        mine = (lane >= h * region) & (lane < (h + 1) * region)
        return jnp.sum(jnp.where(mine, stats, 0.0), axis=-1, keepdims=True)

    new_value = jnp.concatenate([kv_r[pieces + p].astype(F32) for p in range(pieces)], axis=-1)
    new_key = jnp.concatenate([kv_r[p].astype(F32) for p in range(pieces)], axis=-1)
    own_q = q_all[me].astype(F32)
    fresh = [
        jnp.sum(own_q[:, h * HEAD_DIM:(h + 1) * HEAD_DIM] * new_key, axis=-1, keepdims=True) * scale
        for h in range(heads_dev)
    ]

    def top_of(s, tops):
        return tuple(jnp.maximum(t, lse_of(s, h)) for h, t in enumerate(tops))

    tops = lax.fori_loop(0, shards, top_of, tuple(fresh))
    shares = [jnp.exp(f - t) for f, t in zip(fresh, tops)]

    def merge(s, state):
        sums, totals = state
        new_sums, new_totals = [], []
        for h in range(heads_dev):
            share = jnp.exp(lse_of(s, h) - tops[h])
            values = part_r[s, :, h * HEAD_DIM:(h + 1) * HEAD_DIM].astype(F32)
            new_sums.append(sums[h] + share * values)
            new_totals.append(totals[h] + share)
        return tuple(new_sums), tuple(new_totals)

    sums, totals = lax.fori_loop(
        0, shards, merge, (tuple(s * new_value for s in shares), tuple(shares))
    )
    for h in range(heads_dev):
        att_v[:, h * HEAD_DIM:(h + 1) * HEAD_DIM] = (sums[h] / totals[h]).astype(BF16)

    wo_copy.wait()
    out_cols = term_s.shape[2]

    def term_copy(src_slot, dst_slot, peer):
        return pltpu.make_async_remote_copy(
            src_ref=term_s.at[src_slot], dst_ref=term_r.at[dst_slot],
            send_sem=t_send.at[peer], recv_sem=t_recv.at[dst_slot],
            device_id={"seq": peer}, device_id_type=MESH,
        )

    def term_of(d):
        cols = pl.ds(pl.multiple_of(d * out_cols, out_cols), out_cols)
        return jnp.dot(att_v[...], wo_v[:, cols], preferred_element_type=F32)

    def project(i, carry):
        d = lax.rem(me + i, shards)
        term_s[d] = term_of(d).astype(BF16)
        term_copy(d, me, d).start()
        return carry

    lax.fori_loop(1, shards, project, 0)
    own = term_of(me)

    def collect(i, total):
        s = lax.rem(me + i, shards)
        term_copy(s, s, s).wait_recv()
        return total + term_r[s].astype(F32)

    out_ref[...] = lax.fori_loop(1, shards, collect, own).astype(BF16)

    def drain(i, carry):
        peer = lax.rem(me + i, shards)
        q_copy(me, peer).wait_send()
        part_copy(peer, peer, peer).wait_send()
        term_copy(peer, peer, peer).wait_send()
        return carry

    lax.fori_loop(1, shards, drain, 0)
    for g in range(owners):
        peer = my_head * owners + g

        @pl.when(peer != me)
        def _():
            kv_copy(my_slot, peer, g).wait_send()


def body(hidden_in, w_query, w_keyval, key_cache, value_cache, lengths, w_out):
    shards = lax.axis_size("seq")
    batch, depth = hidden_in.shape
    width = w_query.shape[1]
    kv_cols = w_keyval.shape[1]
    heads_dev = width // HEAD_DIM
    owners = shards // KV_HEADS
    group = owners * heads_dev
    pieces = HEAD_DIM // kv_cols
    out_cols = w_out.shape[1] // shards
    chunks = 8
    dma = pltpu.SemaphoreType.DMA
    hbm = pl.BlockSpec(memory_space=pl.ANY)
    return pl.pallas_call(
        functools.partial(kernel, shards, chunks),
        out_shape=jax.ShapeDtypeStruct((batch, out_cols), BF16),
        in_specs=[hbm, hbm, hbm, hbm, hbm, pl.BlockSpec(memory_space=pltpu.SMEM), hbm],
        out_specs=pl.BlockSpec(memory_space=pltpu.VMEM),
        scratch_shapes=[
            pltpu.VMEM(hidden_in.shape, BF16),
            pltpu.VMEM(w_query.shape, BF16),
            pltpu.VMEM(w_keyval.shape, BF16),
            pltpu.VMEM(key_cache.shape, BF16),
            pltpu.VMEM(value_cache.shape, BF16),
            pltpu.VMEM(w_out.shape, BF16),
            pltpu.VMEM((shards, batch, width), BF16),
            pltpu.VMEM((batch, kv_cols), BF16),
            pltpu.VMEM((2 * pieces, batch, kv_cols), BF16),
            pltpu.VMEM((batch, PAIR * group, HEAD_DIM), F32),
            pltpu.VMEM((batch, PAIR * group, HEAD_DIM), F32),
            pltpu.VMEM((batch, PAIR * group, LANES), F32),
            pltpu.VMEM((shards, batch, width + LANES), BF16),
            pltpu.VMEM((shards, batch, width + LANES), BF16),
            pltpu.VMEM((batch, width), BF16),
            pltpu.VMEM((shards, batch, out_cols), BF16),
            pltpu.VMEM((shards, batch, out_cols), BF16),
            dma, dma((chunks,)), dma((chunks,)), dma, dma, dma,
            dma((shards,)), dma((shards,)), dma((owners,)), dma((2 * pieces,)),
            dma((shards,)), dma((shards,)), dma((shards,)), dma((shards,)),
        ],
        compiler_params=pltpu.CompilerParams(
            collective_id=0, has_side_effects=True, vmem_limit_bytes=60 * 1024 * 1024
        ),
    )(hidden_in, w_query, w_keyval, key_cache, value_cache, lengths, w_out)


def solution(mesh):
    placed = (
        P("replica", None),
        P(None, "seq"),
        P(None, "seq"),
        P("replica", "seq", None),
        P("replica", "seq", None),
        P("replica"),
        P("seq", None),
    )
    return jax.shard_map(
        body, mesh=mesh, in_specs=placed, out_specs=P("replica", "seq"), check_vma=False
    )
```

```python
import functools
import math

import jax
import jax.numpy as jnp
from jax import lax
from jax.experimental import pallas as pl
from jax.experimental.pallas import tpu as pltpu
from jax.sharding import PartitionSpec as P

KV_HEADS = 8
HEAD_DIM = 128
LANES = 128
PAIR = 2
MESH = pl.DeviceIdType.MESH
F32 = jnp.float32
BF16 = jnp.bfloat16


def kernel(
    shards, chunks,
    x_hbm, wq_hbm, wkv_hbm, kc_hbm, vc_hbm, len_ref, wo_hbm,
    out_ref,
    x_v, wq_v, wkv_v, kc_v, vc_v, wo_v,
    q_all, kv_s, kv_r, qf, of, lf, part_s, part_r, att_v, term_s, term_r,
    x_sem, wq_sem, wkv_sem, kc_sem, vc_sem, wo_sem,
    q_send, q_relay, q_recv, kv_send, kv_recv, p_send, p_recv, t_send, t_recv,
):
    me = lax.axis_index("seq")
    batch, ctx_dev = kc_v.shape[0], kc_v.shape[1]
    depth = x_v.shape[1]
    width = q_all.shape[2]
    heads_dev = width // HEAD_DIM
    owners = shards // KV_HEADS
    group = owners * heads_dev
    kv_cols = kv_s.shape[1]
    pieces = HEAD_DIM // kv_cols
    step = depth // chunks
    region = LANES // heads_dev

    x_copy = pltpu.make_async_copy(x_hbm, x_v, x_sem)
    x_copy.start()
    wq_copies, wkv_copies = [], []
    for c in range(chunks):
        rows = pl.ds(c * step, step)
        wq_copies.append(pltpu.make_async_copy(wq_hbm.at[rows], wq_v.at[rows], wq_sem.at[c]))
        wkv_copies.append(pltpu.make_async_copy(wkv_hbm.at[rows], wkv_v.at[rows], wkv_sem.at[c]))
        wq_copies[c].start()
        wkv_copies[c].start()
    kc_copy = pltpu.make_async_copy(kc_hbm, kc_v, kc_sem)
    vc_copy = pltpu.make_async_copy(vc_hbm, vc_v, vc_sem)
    wo_copy = pltpu.make_async_copy(wo_hbm, wo_v, wo_sem)

    barrier = pltpu.get_barrier_semaphore()

    def greet(i, carry):
        pl.semaphore_signal(
            barrier, inc=1, device_id={"seq": lax.rem(me + i, shards)}, device_id_type=MESH
        )
        return carry

    lax.fori_loop(1, shards, greet, 0)

    acc_q = jnp.zeros((batch, width), F32)
    acc_kv = jnp.zeros((batch, kv_cols), F32)
    x_copy.wait()
    for c in range(chunks):
        wq_copies[c].wait()
        wkv_copies[c].wait()
        part = x_v[:, c * step:(c + 1) * step]
        acc_q += jnp.dot(part, wq_v[c * step:(c + 1) * step, :], preferred_element_type=F32)
        acc_kv += jnp.dot(part, wkv_v[c * step:(c + 1) * step, :], preferred_element_type=F32)
        if c == chunks // 2:
            kc_copy.start()
            vc_copy.start()
            wo_copy.start()
    q_all[me] = acc_q.astype(BF16)
    kv_s[...] = acc_kv.astype(BF16)

    pl.semaphore_wait(barrier, shards - 1)

    core = lax.rem(me, 2)
    partner = me + 1 - 2 * core

    def q_copy(slot, peer, sem):
        return pltpu.make_async_remote_copy(
            src_ref=q_all.at[slot], dst_ref=q_all.at[slot],
            send_sem=sem, recv_sem=q_recv.at[slot],
            device_id={"seq": peer}, device_id_type=MESH,
        )

    def same_core(i):
        return lax.rem(me + 2 * i, shards)

    def send_q(i, carry):
        peer = same_core(i)
        q_copy(me, peer, q_send.at[peer]).start()
        return carry

    lax.fori_loop(1, shards // 2, send_q, 0)
    q_copy(me, partner, q_send.at[partner]).start()

    half = shards // 2
    role = me // half
    within = me - role * half
    my_head = within // pieces
    my_slot = role * pieces + (within - my_head * pieces)

    def kv_copy(slot, peer, g):
        return pltpu.make_async_remote_copy(
            src_ref=kv_s, dst_ref=kv_r.at[slot],
            send_sem=kv_send.at[g], recv_sem=kv_recv.at[slot],
            device_id={"seq": peer}, device_id_type=MESH,
        )

    def kv_local():
        return pltpu.make_async_copy(kv_s, kv_r.at[my_slot], kv_recv.at[my_slot])

    for g in range(owners):
        peer = my_head * owners + g

        @pl.when(peer != me)
        def _():
            kv_copy(my_slot, peer, g).start()

        @pl.when(peer == me)
        def _():
            kv_local().start()

    kc_copy.wait()
    vc_copy.wait()

    first = me * ctx_dev
    scale = 1.0 / math.sqrt(HEAD_DIM)
    my_group = me // owners
    slots = lax.broadcasted_iota(jnp.int32, (PAIR * group, ctx_dev), 1) + first
    used = jnp.stack([slots < len_ref[b] for b in range(batch)])
    row_head = lax.broadcasted_iota(jnp.int32, (PAIR * group, HEAD_DIM), 0) // group
    lane = lax.broadcasted_iota(jnp.int32, (batch, LANES), 1)

    def part_copy(src_slot, dst_slot, peer):
        return pltpu.make_async_remote_copy(
            src_ref=part_s.at[src_slot], dst_ref=part_r.at[dst_slot],
            send_sem=p_send.at[peer], recv_sem=p_recv.at[dst_slot],
            device_id={"seq": peer}, device_id_type=MESH,
        )

    def part_local():
        return pltpu.make_async_copy(part_s.at[me], part_r.at[me], p_recv.at[me])

    devices = PAIR * owners
    steps = KV_HEADS // PAIR

    def pair_of(i):
        return lax.rem(my_group // PAIR + i, steps)

    def relay(pair):
        def one(g, c):
            src = pair * devices + 2 * g + core

            @pl.when(src != me)
            def _():
                forward = q_copy(src, partner, q_relay.at[src])
                forward.wait_recv()
                forward.start()

            return c

        lax.fori_loop(0, devices // 2, one, 0)

    relay(pair_of(0))

    def attend(i, carry):
        pair = pair_of(i)
        cols = pl.ds(pl.multiple_of(pair * PAIR * HEAD_DIM, PAIR * HEAD_DIM), PAIR * HEAD_DIM)

        @pl.when(i + 1 < steps)
        def _():
            relay(pair_of(i + 1))

        def wait_q(g, c):
            src = pair * devices + 2 * g + 1 - core
            q_copy(src, partner, q_relay.at[src]).wait_recv()
            return c

        lax.fori_loop(0, devices // 2, wait_q, 0)
        for g in range(devices):
            block = q_all[pair * devices + g].astype(F32)
            for h in range(heads_dev):
                qf[:, g * heads_dev + h, :] = block[:, h * HEAD_DIM:(h + 1) * HEAD_DIM]
        scores = []
        for b in range(batch):
            rows = qf[b]
            wide = jnp.concatenate(
                [jnp.where(row_head == n, rows, 0.0) for n in range(PAIR)], axis=1
            )
            scores.append(lax.dot_general(
                wide.astype(BF16), kc_v[b, :, cols], (((1,), (1,)), ((), ())),
                preferred_element_type=F32,
            ))
        scores = jnp.where(used, jnp.stack(scores) * scale, -1e30)
        largest = jnp.max(scores, axis=-1, keepdims=True)
        weights = jnp.exp(scores - largest)
        total = jnp.sum(weights, axis=-1, keepdims=True)
        lf[...] = jnp.broadcast_to(largest + jnp.log(total), lf.shape)
        inverse = 1.0 / total
        weights = weights.astype(BF16)
        for b in range(batch):
            summed = jnp.dot(weights[b], vc_v[b, :, cols], preferred_element_type=F32)
            mine = [
                summed[n * group:(n + 1) * group, n * HEAD_DIM:(n + 1) * HEAD_DIM]
                for n in range(PAIR)
            ]
            of[b] = jnp.concatenate(mine, axis=0) * inverse[b]
        for g in range(devices):
            d = pair * devices + g
            stats = jnp.zeros((batch, LANES), F32)
            for h in range(heads_dev):
                part_s[d, :, h * HEAD_DIM:(h + 1) * HEAD_DIM] = of[:, g * heads_dev + h, :].astype(BF16)
                lse = lf[:, g * heads_dev + h, :]
                high = lse.astype(BF16).astype(F32)
                mid = (lse - high).astype(BF16).astype(F32)
                low = lse - high - mid
                base = h * region
                stats = jnp.where(lane == base, high, stats)
                stats = jnp.where(lane == base + 1, mid, stats)
                stats = jnp.where(lane == base + 2, low, stats)
            part_s[d, :, width:] = stats.astype(BF16)

        def send_part(g, c):
            d = pair * devices + g

            @pl.when(d != me)
            def _():
                part_copy(d, me, d).start()

            @pl.when(d == me)
            def _():
                part_local().start()

            return c

        lax.fori_loop(0, devices, send_part, 0)
        return carry

    lax.fori_loop(0, steps, attend, 0)

    owner_head = me // owners
    for r in range(2 * pieces):
        src = (r // pieces) * half + owner_head * pieces + r % pieces

        @pl.when(src != me)
        def _():
            kv_copy(r, src, 0).wait_recv()

        @pl.when(src == me)
        def _():
            kv_local().wait()

    def wait_part(i, carry):
        part_copy(lax.rem(me + i, shards), lax.rem(me + i, shards), lax.rem(me + i, shards)).wait_recv()
        return carry

    lax.fori_loop(1, shards, wait_part, 0)
    part_local().wait()

    new_value = jnp.concatenate([kv_r[pieces + p].astype(F32) for p in range(pieces)], axis=-1)
    new_key = jnp.concatenate([kv_r[p].astype(F32) for p in range(pieces)], axis=-1)
    own_q = q_all[me].astype(F32)
    stats = part_r[:, :, width:].astype(F32)
    lanes = lax.broadcasted_iota(jnp.int32, stats.shape, 2)
    for h in range(heads_dev):
        cols = slice(h * HEAD_DIM, (h + 1) * HEAD_DIM)
        mine = (lanes >= h * region) & (lanes < (h + 1) * region)
        lse = jnp.sum(jnp.where(mine, stats, 0.0), axis=-1, keepdims=True)
        fresh = jnp.sum(own_q[:, cols] * new_key, axis=-1, keepdims=True) * scale
        top = jnp.maximum(jnp.max(lse, axis=0), fresh)
        share = jnp.exp(lse - top[None])
        fresh = jnp.exp(fresh - top)
        summed = jnp.sum(share * part_r[:, :, cols].astype(F32), axis=0) + fresh * new_value
        att_v[:, cols] = (summed / (jnp.sum(share, axis=0) + fresh)).astype(BF16)

    wo_copy.wait()
    out_cols = term_s.shape[2]

    def term_copy(src_slot, dst_slot, peer):
        return pltpu.make_async_remote_copy(
            src_ref=term_s.at[src_slot], dst_ref=term_r.at[dst_slot],
            send_sem=t_send.at[peer], recv_sem=t_recv.at[dst_slot],
            device_id={"seq": peer}, device_id_type=MESH,
        )

    def term_of(d):
        cols = pl.ds(pl.multiple_of(d * out_cols, out_cols), out_cols)
        return jnp.dot(att_v[...], wo_v[:, cols], preferred_element_type=F32)

    burst = 3 if (shards - 1) % 3 == 0 else 1

    def project(i, carry):
        targets = [lax.rem(me + 1 + i * burst + j, shards) for j in range(burst)]
        terms = [term_of(d) for d in targets]
        for d, term in zip(targets, terms):
            term_s[d] = term.astype(BF16)
        for d in targets:
            term_copy(d, me, d).start()
        return carry

    lax.fori_loop(0, (shards - 1) // burst, project, 0)
    term_r[me] = term_of(me).astype(BF16)

    def collect(i, carry):
        s = lax.rem(me + i, shards)
        term_copy(s, s, s).wait_recv()
        return carry

    lax.fori_loop(1, shards, collect, 0)
    out_ref[...] = jnp.sum(term_r[...].astype(F32), axis=0).astype(BF16)

    def drain(i, carry):
        peer = lax.rem(me + i, shards)
        part_copy(peer, peer, peer).wait_send()
        term_copy(peer, peer, peer).wait_send()
        return carry

    lax.fori_loop(1, shards, drain, 0)

    def drain_q(i, carry):
        peer = same_core(i)
        q_copy(me, peer, q_send.at[peer]).wait_send()
        q_copy(peer, partner, q_relay.at[peer]).wait_send()
        return carry

    lax.fori_loop(1, shards // 2, drain_q, 0)
    q_copy(me, partner, q_send.at[partner]).wait_send()
    for g in range(owners):
        peer = my_head * owners + g

        @pl.when(peer != me)
        def _():
            kv_copy(my_slot, peer, g).wait_send()


def body(hidden_in, w_query, w_keyval, key_cache, value_cache, lengths, w_out):
    shards = lax.axis_size("seq")
    batch, depth = hidden_in.shape
    width = w_query.shape[1]
    kv_cols = w_keyval.shape[1]
    heads_dev = width // HEAD_DIM
    owners = shards // KV_HEADS
    group = owners * heads_dev
    pieces = HEAD_DIM // kv_cols
    out_cols = w_out.shape[1] // shards
    chunks = 8
    dma = pltpu.SemaphoreType.DMA
    hbm = pl.BlockSpec(memory_space=pl.ANY)
    return pl.pallas_call(
        functools.partial(kernel, shards, chunks),
        out_shape=jax.ShapeDtypeStruct((batch, out_cols), BF16),
        in_specs=[hbm, hbm, hbm, hbm, hbm, pl.BlockSpec(memory_space=pltpu.SMEM), hbm],
        out_specs=pl.BlockSpec(memory_space=pltpu.VMEM),
        scratch_shapes=[
            pltpu.VMEM(hidden_in.shape, BF16),
            pltpu.VMEM(w_query.shape, BF16),
            pltpu.VMEM(w_keyval.shape, BF16),
            pltpu.VMEM(key_cache.shape, BF16),
            pltpu.VMEM(value_cache.shape, BF16),
            pltpu.VMEM(w_out.shape, BF16),
            pltpu.VMEM((shards, batch, width), BF16),
            pltpu.VMEM((batch, kv_cols), BF16),
            pltpu.VMEM((2 * pieces, batch, kv_cols), BF16),
            pltpu.VMEM((batch, PAIR * group, HEAD_DIM), F32),
            pltpu.VMEM((batch, PAIR * group, HEAD_DIM), F32),
            pltpu.VMEM((batch, PAIR * group, LANES), F32),
            pltpu.VMEM((shards, batch, width + LANES), BF16),
            pltpu.VMEM((shards, batch, width + LANES), BF16),
            pltpu.VMEM((batch, width), BF16),
            pltpu.VMEM((shards, batch, out_cols), BF16),
            pltpu.VMEM((shards, batch, out_cols), BF16),
            dma, dma((chunks,)), dma((chunks,)), dma, dma, dma,
            dma((shards,)), dma((shards,)), dma((shards,)), dma((owners,)), dma((2 * pieces,)),
            dma((shards,)), dma((shards,)), dma((shards,)), dma((shards,)),
        ],
        compiler_params=pltpu.CompilerParams(
            collective_id=0, has_side_effects=True, vmem_limit_bytes=60 * 1024 * 1024
        ),
    )(hidden_in, w_query, w_keyval, key_cache, value_cache, lengths, w_out)


def solution(mesh):
    placed = (
        P("replica", None),
        P(None, "seq"),
        P(None, "seq"),
        P("replica", "seq", None),
        P("replica", "seq", None),
        P("replica"),
        P("seq", None),
    )
    return jax.shard_map(
        body, mesh=mesh, in_specs=placed, out_specs=P("replica", "seq"), check_vma=False
    )
```

```python
import functools
import math

import jax
import jax.numpy as jnp
from jax import lax
from jax.experimental import pallas as pl
from jax.experimental.pallas import tpu as pltpu
from jax.sharding import PartitionSpec as P

KV_HEADS = 8
HEAD_DIM = 128
LANES = 128
PAIR = 2
MESH = pl.DeviceIdType.MESH
F32 = jnp.float32
BF16 = jnp.bfloat16


def kernel(
    shards, chunks,
    x_hbm, wq_hbm, wkv_hbm, kc_hbm, vc_hbm, len_ref, wo_hbm,
    out_ref,
    x_v, wq_v, wkv_v, kc_v, vc_v, wo_v,
    q_all, kv_s, kv_r, qf, of, lf, part_s, part_r, att_v, term_s, term_r,
    x_sem, wq_sem, wkv_sem, kc_sem, vc_sem, wo_sem,
    q_send, q_relay, q_recv, kv_send, kv_recv, p_send, p_recv, t_send, t_recv, h_send, h_recv, half_r,
):
    me = lax.axis_index("seq")
    batch, ctx_dev = kc_v.shape[0], kc_v.shape[1]
    depth = x_v.shape[1]
    width = q_all.shape[2]
    heads_dev = width // HEAD_DIM
    owners = shards // KV_HEADS
    group = owners * heads_dev
    kv_cols = kv_s.shape[1]
    pieces = HEAD_DIM // kv_cols
    step = depth // chunks
    region = LANES // heads_dev

    x_copy = pltpu.make_async_copy(x_hbm, x_v, x_sem)
    x_copy.start()
    wq_copies, wkv_copies = [], []
    for c in range(chunks):
        rows = pl.ds(c * step, step)
        wq_copies.append(pltpu.make_async_copy(wq_hbm.at[rows], wq_v.at[rows], wq_sem.at[c]))
        wkv_copies.append(pltpu.make_async_copy(wkv_hbm.at[rows], wkv_v.at[rows], wkv_sem.at[c]))
        wq_copies[c].start()
        wkv_copies[c].start()
    kc_copy = pltpu.make_async_copy(kc_hbm, kc_v, kc_sem)
    vc_copy = pltpu.make_async_copy(vc_hbm, vc_v, vc_sem)
    wo_copy = pltpu.make_async_copy(wo_hbm, wo_v, wo_sem)

    barrier = pltpu.get_barrier_semaphore()

    def greet(i, carry):
        pl.semaphore_signal(
            barrier, inc=1, device_id={"seq": lax.rem(me + i, shards)}, device_id_type=MESH
        )
        return carry

    lax.fori_loop(1, shards, greet, 0)

    acc_q = jnp.zeros((batch, width), F32)
    acc_kv = jnp.zeros((batch, kv_cols), F32)
    x_copy.wait()
    for c in range(chunks):
        wq_copies[c].wait()
        wkv_copies[c].wait()
        part = x_v[:, c * step:(c + 1) * step]
        acc_q += jnp.dot(part, wq_v[c * step:(c + 1) * step, :], preferred_element_type=F32)
        acc_kv += jnp.dot(part, wkv_v[c * step:(c + 1) * step, :], preferred_element_type=F32)
        if c == chunks // 2:
            kc_copy.start()
            vc_copy.start()
            wo_copy.start()
    q_all[me] = acc_q.astype(BF16)
    kv_s[...] = acc_kv.astype(BF16)

    pl.semaphore_wait(barrier, shards - 1)

    core = lax.rem(me, 2)
    partner = me + 1 - 2 * core

    def q_copy(slot, peer, sem):
        return pltpu.make_async_remote_copy(
            src_ref=q_all.at[slot], dst_ref=q_all.at[slot],
            send_sem=sem, recv_sem=q_recv.at[slot],
            device_id={"seq": peer}, device_id_type=MESH,
        )

    def same_core(i):
        return lax.rem(me + 2 * i, shards)

    def send_q(i, carry):
        peer = same_core(i)
        q_copy(me, peer, q_send.at[peer]).start()
        return carry

    lax.fori_loop(1, shards // 2, send_q, 0)
    q_copy(me, partner, q_send.at[partner]).start()

    half = shards // 2
    role = me // half
    within = me - role * half
    my_head = within // pieces
    my_slot = role * pieces + (within - my_head * pieces)

    def kv_copy(slot, peer, g):
        return pltpu.make_async_remote_copy(
            src_ref=kv_s, dst_ref=kv_r.at[slot],
            send_sem=kv_send.at[g], recv_sem=kv_recv.at[slot],
            device_id={"seq": peer}, device_id_type=MESH,
        )

    def kv_local():
        return pltpu.make_async_copy(kv_s, kv_r.at[my_slot], kv_recv.at[my_slot])

    for g in range(owners):
        peer = my_head * owners + g

        @pl.when(peer != me)
        def _():
            kv_copy(my_slot, peer, g).start()

        @pl.when(peer == me)
        def _():
            kv_local().start()

    kc_copy.wait()
    vc_copy.wait()

    first = me * ctx_dev
    scale = 1.0 / math.sqrt(HEAD_DIM)
    my_group = me // owners
    slots = lax.broadcasted_iota(jnp.int32, (PAIR * group, ctx_dev), 1) + first
    used = jnp.stack([slots < len_ref[b] for b in range(batch)])
    row_head = lax.broadcasted_iota(jnp.int32, (PAIR * group, HEAD_DIM), 0) // group
    lane = lax.broadcasted_iota(jnp.int32, (batch, LANES), 1)

    def part_copy(src_slot, dst_slot, peer):
        return pltpu.make_async_remote_copy(
            src_ref=part_s.at[src_slot], dst_ref=part_r.at[dst_slot],
            send_sem=p_send.at[peer], recv_sem=p_recv.at[dst_slot],
            device_id={"seq": peer}, device_id_type=MESH,
        )

    def part_local():
        return pltpu.make_async_copy(part_s.at[me], part_r.at[me], p_recv.at[me])

    devices = PAIR * owners
    steps = KV_HEADS // PAIR

    def pair_of(i):
        return lax.rem(my_group // PAIR + i, steps)

    def relay(pair):
        def one(g, c):
            src = pair * devices + 2 * g + core

            @pl.when(src != me)
            def _():
                forward = q_copy(src, partner, q_relay.at[src])
                forward.wait_recv()
                forward.start()

            return c

        lax.fori_loop(0, devices // 2, one, 0)

    relay(pair_of(0))

    def attend(i, carry):
        pair = pair_of(i)
        cols = pl.ds(pl.multiple_of(pair * PAIR * HEAD_DIM, PAIR * HEAD_DIM), PAIR * HEAD_DIM)

        @pl.when(i + 1 < steps)
        def _():
            relay(pair_of(i + 1))

        def wait_q(g, c):
            src = pair * devices + 2 * g + 1 - core
            q_copy(src, partner, q_relay.at[src]).wait_recv()
            return c

        lax.fori_loop(0, devices // 2, wait_q, 0)
        for g in range(devices):
            block = q_all[pair * devices + g].astype(F32)
            for h in range(heads_dev):
                qf[:, g * heads_dev + h, :] = block[:, h * HEAD_DIM:(h + 1) * HEAD_DIM]
        scores = []
        for b in range(batch):
            rows = qf[b]
            wide = jnp.concatenate(
                [jnp.where(row_head == n, rows, 0.0) for n in range(PAIR)], axis=1
            )
            scores.append(lax.dot_general(
                wide.astype(BF16), kc_v[b, :, cols], (((1,), (1,)), ((), ())),
                preferred_element_type=F32,
            ))
        scores = jnp.where(used, jnp.stack(scores) * scale, -1e30)
        largest = jnp.max(scores, axis=-1, keepdims=True)
        weights = jnp.exp(scores - largest)
        total = jnp.sum(weights, axis=-1, keepdims=True)
        lf[...] = jnp.broadcast_to(largest + jnp.log(total), lf.shape)
        inverse = 1.0 / total
        weights = weights.astype(BF16)
        for b in range(batch):
            summed = jnp.dot(weights[b], vc_v[b, :, cols], preferred_element_type=F32)
            mine = [
                summed[n * group:(n + 1) * group, n * HEAD_DIM:(n + 1) * HEAD_DIM]
                for n in range(PAIR)
            ]
            of[b] = jnp.concatenate(mine, axis=0) * inverse[b]
        for g in range(devices):
            d = pair * devices + g
            stats = jnp.zeros((batch, LANES), F32)
            for h in range(heads_dev):
                part_s[d, :, h * HEAD_DIM:(h + 1) * HEAD_DIM] = of[:, g * heads_dev + h, :].astype(BF16)
                lse = lf[:, g * heads_dev + h, :]
                high = lse.astype(BF16).astype(F32)
                mid = (lse - high).astype(BF16).astype(F32)
                low = lse - high - mid
                base = h * region
                stats = jnp.where(lane == base, high, stats)
                stats = jnp.where(lane == base + 1, mid, stats)
                stats = jnp.where(lane == base + 2, low, stats)
            part_s[d, :, width:] = stats.astype(BF16)

        def send_part(g, c):
            d = pair * devices + g

            @pl.when(d != me)
            def _():
                part_copy(d, me, d).start()

            @pl.when(d == me)
            def _():
                part_local().start()

            return c

        lax.fori_loop(0, devices, send_part, 0)
        return carry

    lax.fori_loop(0, steps, attend, 0)

    owner_head = me // owners
    for r in range(2 * pieces):
        src = (r // pieces) * half + owner_head * pieces + r % pieces

        @pl.when(src != me)
        def _():
            kv_copy(r, src, 0).wait_recv()

        @pl.when(src == me)
        def _():
            kv_local().wait()

    def wait_part(i, carry):
        part_copy(lax.rem(me + i, shards), lax.rem(me + i, shards), lax.rem(me + i, shards)).wait_recv()
        return carry

    lax.fori_loop(1, shards, wait_part, 0)
    part_local().wait()

    new_value = jnp.concatenate([kv_r[pieces + p].astype(F32) for p in range(pieces)], axis=-1)
    new_key = jnp.concatenate([kv_r[p].astype(F32) for p in range(pieces)], axis=-1)
    own_q = q_all[me].astype(F32)
    stats = part_r[:, :, width:].astype(F32)
    lanes = lax.broadcasted_iota(jnp.int32, stats.shape, 2)
    for h in range(heads_dev):
        cols = slice(h * HEAD_DIM, (h + 1) * HEAD_DIM)
        mine = (lanes >= h * region) & (lanes < (h + 1) * region)
        lse = jnp.sum(jnp.where(mine, stats, 0.0), axis=-1, keepdims=True)
        fresh = jnp.sum(own_q[:, cols] * new_key, axis=-1, keepdims=True) * scale
        top = jnp.maximum(jnp.max(lse, axis=0), fresh)
        share = jnp.exp(lse - top[None])
        fresh = jnp.exp(fresh - top)
        summed = jnp.sum(share * part_r[:, :, cols].astype(F32), axis=0) + fresh * new_value
        att_v[:, cols] = (summed / (jnp.sum(share, axis=0) + fresh)).astype(BF16)

    wo_copy.wait()
    out_cols = term_s.shape[2]

    def term_copy(src_slot, dst_slot, peer):
        return pltpu.make_async_remote_copy(
            src_ref=term_s.at[src_slot], dst_ref=term_r.at[dst_slot],
            send_sem=t_send.at[peer], recv_sem=t_recv.at[dst_slot],
            device_id={"seq": peer}, device_id_type=MESH,
        )

    def term_of(d):
        cols = pl.ds(pl.multiple_of(d * out_cols, out_cols), out_cols)
        return jnp.dot(att_v[...], wo_v[:, cols], preferred_element_type=F32)

    def half_copy(d):
        return pltpu.make_async_remote_copy(
            src_ref=term_s.at[d], dst_ref=half_r.at[d],
            send_sem=h_send.at[d], recv_sem=h_recv.at[d],
            device_id={"seq": partner}, device_id_type=MESH,
        )

    burst = 4

    def project_other(i, carry):
        targets = [lax.rem(partner + 2 * (1 + i * burst + j), shards) for j in range(burst)]
        terms = [term_of(d) for d in targets]
        for d, term in zip(targets, terms):
            term_s[d] = term.astype(BF16)
        for d in targets:
            half_copy(d).start()
        return carry

    lax.fori_loop(0, shards // 2 // burst, project_other, 0)

    def project(i, carry):
        targets = [lax.rem(me + 2 * (1 + i * burst + j), shards) for j in range(burst)]
        terms = [term_of(d) for d in targets]
        for d in targets:
            half_copy(d).wait_recv()
        for d, term in zip(targets, terms):
            term_s[d] = (term + half_r[d].astype(F32)).astype(BF16)
        for d in targets:
            @pl.when(d != me)
            def _():
                term_copy(d, me // 2, d).start()
        return carry

    lax.fori_loop(0, shards // 2 // burst, project, 0)
    term_r[me // 2] = term_s[me]

    def collect(i, carry):
        s = same_core(i)
        term_copy(s, s // 2, s).wait_recv()
        return carry

    lax.fori_loop(1, shards // 2, collect, 0)
    out_ref[...] = jnp.sum(term_r[...].astype(F32), axis=0).astype(BF16)

    def drain(i, carry):
        peer = lax.rem(me + i, shards)
        part_copy(peer, peer, peer).wait_send()
        return carry

    lax.fori_loop(1, shards, drain, 0)

    def drain_q(i, carry):
        peer = same_core(i)
        q_copy(me, peer, q_send.at[peer]).wait_send()
        term_copy(peer, peer // 2, peer).wait_send()
        q_copy(peer, partner, q_relay.at[peer]).wait_send()
        return carry

    lax.fori_loop(1, shards // 2, drain_q, 0)

    def drain_half(i, carry):
        half_copy(lax.rem(partner + 2 * i, shards)).wait_send()
        return carry

    lax.fori_loop(0, shards // 2, drain_half, 0)
    q_copy(me, partner, q_send.at[partner]).wait_send()
    for g in range(owners):
        peer = my_head * owners + g

        @pl.when(peer != me)
        def _():
            kv_copy(my_slot, peer, g).wait_send()


def body(hidden_in, w_query, w_keyval, key_cache, value_cache, lengths, w_out):
    shards = lax.axis_size("seq")
    batch, depth = hidden_in.shape
    width = w_query.shape[1]
    kv_cols = w_keyval.shape[1]
    heads_dev = width // HEAD_DIM
    owners = shards // KV_HEADS
    group = owners * heads_dev
    pieces = HEAD_DIM // kv_cols
    out_cols = w_out.shape[1] // shards
    chunks = 8
    dma = pltpu.SemaphoreType.DMA
    hbm = pl.BlockSpec(memory_space=pl.ANY)
    return pl.pallas_call(
        functools.partial(kernel, shards, chunks),
        out_shape=jax.ShapeDtypeStruct((batch, out_cols), BF16),
        in_specs=[hbm, hbm, hbm, hbm, hbm, pl.BlockSpec(memory_space=pltpu.SMEM), hbm],
        out_specs=pl.BlockSpec(memory_space=pltpu.VMEM),
        scratch_shapes=[
            pltpu.VMEM(hidden_in.shape, BF16),
            pltpu.VMEM(w_query.shape, BF16),
            pltpu.VMEM(w_keyval.shape, BF16),
            pltpu.VMEM(key_cache.shape, BF16),
            pltpu.VMEM(value_cache.shape, BF16),
            pltpu.VMEM(w_out.shape, BF16),
            pltpu.VMEM((shards, batch, width), BF16),
            pltpu.VMEM((batch, kv_cols), BF16),
            pltpu.VMEM((2 * pieces, batch, kv_cols), BF16),
            pltpu.VMEM((batch, PAIR * group, HEAD_DIM), F32),
            pltpu.VMEM((batch, PAIR * group, HEAD_DIM), F32),
            pltpu.VMEM((batch, PAIR * group, LANES), F32),
            pltpu.VMEM((shards, batch, width + LANES), BF16),
            pltpu.VMEM((shards, batch, width + LANES), BF16),
            pltpu.VMEM((batch, width), BF16),
            pltpu.VMEM((shards, batch, out_cols), BF16),
            pltpu.VMEM((shards // 2, batch, out_cols), BF16),
            dma, dma((chunks,)), dma((chunks,)), dma, dma, dma,
            dma((shards,)), dma((shards,)), dma((shards,)), dma((owners,)), dma((2 * pieces,)),
            dma((shards,)), dma((shards,)), dma((shards,)), dma((shards,)),
            dma((shards,)), dma((shards,)), pltpu.VMEM((shards, batch, out_cols), BF16),
        ],
        compiler_params=pltpu.CompilerParams(
            collective_id=0, has_side_effects=True, vmem_limit_bytes=60 * 1024 * 1024
        ),
    )(hidden_in, w_query, w_keyval, key_cache, value_cache, lengths, w_out)


def solution(mesh):
    placed = (
        P("replica", None),
        P(None, "seq"),
        P(None, "seq"),
        P("replica", "seq", None),
        P("replica", "seq", None),
        P("replica"),
        P("seq", None),
    )
    return jax.shard_map(
        body, mesh=mesh, in_specs=placed, out_specs=P("replica", "seq"), check_vma=False
    )
```
